128 devices in a mesh: bank: 4 (over y_lo, core), zero: 32 (over z, y_hi, x).
Axes of the slice: x: 4, y: 4 (y_hi: 2, y_lo: 2; y = y_hi * 2 + y_lo), z: 4, core: 2. Of those that a mesh axis runs over, the one named last changes fastest.
Arguments:
- master_down: float32 [16, 6400, 4096], P('bank', None, 'zero'), may hold values from -0.078125 to 0.078125
- router_weight: float32 [4096, 16], P('zero', 'bank'), may hold values from -0.09375 to 0.09375
- router_gain: float32 [4096], P('zero'), may hold values from 0.25 to 1.75
Outputs:
- final_down: bfloat16 [16, 4096, 6400], P('bank', None, 'zero')
- serve_router: bfloat16 [4096, 16], replicated
The draws below stay inside these ranges and needn't reach their ends.
All inputs are finite; a program needn't handle non-finite values.
Results may differ from the reference program's by a relative error of at most 0.001.
Values may be sent and summed in bfloat16 or wider, within the bound.
No kernel may reach another device: no remote copies, remote signals or barrier semaphores. Data moves between devices by JAX's collectives and lax.ppermute only.
A program may use at most 128 MiB of HBM per device.

```python
import jax
import jax.numpy as jnp

EXPERTS = 16
D_MODEL = 4096
D_EXPERT = 6400


def block_scale(stream_key, shape, split, smallest, high):
    def one(dim, shards_of):
        draws = jax.random.uniform(jax.random.fold_in(jax.random.fold_in(stream_key, 6), dim), (shards_of,), jnp.float32, smallest / len(split), high / len(split))
        return jnp.repeat(jnp.exp(draws), shape[dim] // shards_of).reshape((-1,) + (1,) * (len(shape) - dim - 1))

    level = one(*split[0])
    for cut in split[1:]:
        level = level * one(*cut)
    return level


def bell_draw(own_key, dims, deviation, bound, pieces=(), dtype=jnp.bfloat16):
    factor_of = block_scale(own_key, dims, pieces, -0.22, 0.18) if pieces else 1.0
    array = jax.random.normal(own_key, dims, jnp.float32) * deviation * factor_of
    return jnp.minimum(jnp.maximum(array, -bound), bound).astype(dtype)


def setup_inputs(seed: int = 0) -> dict:
    splits = jax.random.split(jax.random.key(seed), 4)
    master_down = bell_draw(splits[0], (EXPERTS, D_EXPERT, D_MODEL), D_EXPERT ** -0.5, 0.078125, ((0, 4), (2, 32)), jnp.float32)
    router_weight = bell_draw(splits[1], (D_MODEL, EXPERTS), D_MODEL ** -0.5, 0.09375, ((0, 32), (1, 4)), jnp.float32)
    router_gain = jnp.clip(1.0 + 0.15 * jax.random.normal(splits[2], (D_MODEL,), jnp.float32), 0.25, 1.75)
    return {"master_down": master_down, "router_weight": router_weight, "router_gain": router_gain}


def reference(master_down, router_weight, router_gain):
    final_down = master_down.astype(jnp.bfloat16)
    final_down = jnp.transpose(final_down, (0, 2, 1))
    serve_router = (router_weight * router_gain[:, None]).astype(jnp.bfloat16)
    return final_down, serve_router
```

```python
import functools

import jax
import jax.numpy as jnp
from jax import lax
from jax.experimental import pallas as pl
from jax.experimental.pallas import tpu as pltpu
from jax.sharding import PartitionSpec as P

CHUNKS = ((0, 1), (1, 4))
Z, Y, X = 4, 2, 4
PEERS = Z * Y * X
LISTED = [z * Y * X + y * X + x for x in range(X) for y in range(Y) for z in range(Z)]
BANKS = 4


def narrow_kernel(first, count, rows, slots, down, *rest):
    router, out, wide, slim, come, go, sem = rest if len(rest) == 7 else (None, *rest)
    lump = Y * X * rows
    steps = [(e, z) for e in range(count) for z in range(Z)]

    def fetch(k):
        e, z = steps[k]
        return pltpu.make_async_copy(
            down.at[first + e, pl.ds(z * lump, lump)], wide.at[k % slots], come.at[k % slots]
        )

    def put(k):
        e, z = steps[k]
        return pltpu.make_async_copy(
            slim.at[k % slots], out.at[:, z, pl.ds(e * rows, rows)], go.at[k % slots]
        )

    for k in range(min(slots, len(steps))):
        fetch(k).start()
    if router is not None:
        tail = router.shape[0]
        spread = [
            pltpu.make_async_copy(router, out.at[n, z, pl.ds(count * rows, tail)], sem)
            for n in range(X * Y)
            for z in range(Z)
        ]
        for c in spread:
            c.start()
    for k in range(len(steps)):
        if k >= slots:
            put(k - slots).wait()
        fetch(k).wait()
        for y in range(Y):
            for x in range(X):
                piece = wide[k % slots, pl.ds((y * X + x) * rows, rows)]
                slim[k % slots, x * Y + y] = piece.astype(jnp.bfloat16)
        put(k).start()
        if k + slots < len(steps):
            fetch(k + slots).start()
    for k in range(max(0, len(steps) - slots), len(steps)):
        put(k).wait()
    if router is not None:
        for c in spread:
            c.wait()


def narrow(down, first, last, router=None):
    count, rows = last - first, down.shape[1] // PEERS
    tail = 0 if router is None else router.shape[0]
    slots = 3
    down = pltpu.with_memory_space_constraint(down, pltpu.HBM)
    given = (down,) if router is None else (down, router)
    hbm = pl.BlockSpec(memory_space=pltpu.HBM)
    out = pl.pallas_call(
        functools.partial(narrow_kernel, first, count, rows, slots),
        out_shape=pltpu.HBM((X * Y, Z, count * rows + tail, 128), jnp.bfloat16),
        in_specs=[hbm] + [pl.BlockSpec(memory_space=pltpu.VMEM)] * (len(given) - 1),
        out_specs=hbm,
        scratch_shapes=[
            pltpu.VMEM((slots, Y * X * rows, 128), jnp.float32),
            pltpu.VMEM((slots, X * Y, rows, 128), jnp.bfloat16),
            pltpu.SemaphoreType.DMA((slots,)),
            pltpu.SemaphoreType.DMA((slots,)),
            pltpu.SemaphoreType.DMA,
        ],
        compiler_params=pltpu.CompilerParams(vmem_limit_bytes=8 << 20),
        cost_estimate=pl.CostEstimate(
            flops=count * PEERS * rows * 128 * 40,
            bytes_accessed=count * PEERS * rows * 128 * 6,
            transcendentals=0,
        ),
    )(*given)
    return out.reshape(PEERS, count * rows + tail, 128)


def place_kernel(first, count, rows, tail, aliased, got, *rest):
    rest = rest[1:] if aliased else rest
    final, serve, sem = rest if tail else (rest[0], None, rest[1])
    copies = []
    for at, p in enumerate(LISTED):
        columns = pl.ds(p * 128, 128)
        for e in range(count):
            copies.append((got.at[at, pl.ds(e * rows, rows)], final.at[first + e, :, columns]))
        if tail:
            copies.append((got.at[at, pl.ds(count * rows, tail)], serve.at[:, columns]))
    copies = [pltpu.make_async_copy(a, b, sem) for a, b in copies]
    for c in copies:
        c.start()
    for c in copies:
        c.wait()


def place(got, first, last, experts, rows, tail, final=None):
    count = last - first
    anywhere = pl.BlockSpec(memory_space=pltpu.HBM)
    shapes = [pltpu.HBM((experts, rows, PEERS * 128), jnp.bfloat16)]
    if tail:
        shapes.append(pltpu.HBM((tail, PEERS * 128), jnp.bfloat16))
    got = pltpu.with_memory_space_constraint(got, pltpu.VMEM)
    given = (got,) if final is None else (got, final)
    return pl.pallas_call(
        functools.partial(place_kernel, first, count, rows, tail, final is not None),
        out_shape=shapes,
        in_specs=[pl.BlockSpec(memory_space=pltpu.VMEM)] + [anywhere] * (len(given) - 1),
        out_specs=[anywhere] * len(shapes),
        scratch_shapes=[pltpu.SemaphoreType.DMA],
        input_output_aliases={} if final is None else {1: 0},
        compiler_params=pltpu.CompilerParams(vmem_limit_bytes=8 << 20),
        cost_estimate=pl.CostEstimate(
            flops=count * PEERS * rows * 128 * 20, bytes_accessed=count * PEERS * rows * 128 * 4, transcendentals=0
        ),
    )(*given)


def all_banks(part):
    me = lax.axis_index("bank")
    by_step = [part] + [
        lax.ppermute(part, "bank", [(b, b ^ k) for b in range(BANKS)]) for k in range(1, BANKS)
    ]
    blocks = []
    for g in range(BANKS):
        block = by_step[g]
        for b in range(1, BANKS):
            block = jnp.where(me == b, by_step[g ^ b], block)
        blocks.append(block)
    return jnp.concatenate(blocks, axis=0)


def exchange(sent):
    return lax.all_to_all(sent, "zero", 0, 0, axis_index_groups=[LISTED], tiled=True)


def body(master_down, router_weight, router_gain):
    experts, rows = master_down.shape[0], master_down.shape[1] // PEERS
    part = (router_weight.T * router_gain[None, :]).astype(jnp.bfloat16)
    router = all_banks(part)
    got = []
    for k, (first, last) in enumerate(CHUNKS):
        with_router = router if k == len(CHUNKS) - 1 else None
        got.append(exchange(narrow(master_down, first, last, with_router)))
    final = None
    for k, (first, last) in enumerate(CHUNKS):
        tail = router.shape[0] if k == len(CHUNKS) - 1 else 0
        final, *serve = place(got[k], first, last, experts, rows, tail, final)
    return jnp.transpose(final, (0, 2, 1)), serve[0].T


def solution(mesh):
    placed = (P("bank", None, "zero"), P("zero", "bank"), P("zero"))
    return jax.shard_map(
        body, mesh=mesh, in_specs=placed, out_specs=(P("bank", None, "zero"), P()), check_vma=False
    )
```

```python
import functools

import jax
import jax.numpy as jnp
from jax import lax
from jax.experimental import pallas as pl
from jax.experimental.pallas import tpu as pltpu
from jax.sharding import PartitionSpec as P

Z, Y, X = 4, 2, 4
PEERS = Z * Y * X
LISTED = [z * Y * X + y * X + x for z in range(Z) for x in range(X) for y in range(Y)]
BANKS = 4
LANES = 128
HBM = pl.BlockSpec(memory_space=pltpu.HBM)
VMEM = pl.BlockSpec(memory_space=pltpu.VMEM)


def narrow_kernel(experts, rows, down, out, wide, slim, come, go):
    lump = Y * X * rows
    steps = [(e, z) for e in range(experts) for z in range(Z)]

    def fetch(k):
        e, z = steps[k]
        return pltpu.make_async_copy(
            down.at[e, pl.ds(z * lump, lump)], wide.at[k], come.at[k]
        )

    def put(k):
        e, z = steps[k]
        return pltpu.make_async_copy(
            slim.at[k], out.at[z, :, pl.ds(e * rows, rows)], go.at[k]
        )

    for k in range(len(steps)):
        fetch(k).start()
    for k in range(len(steps)):
        fetch(k).wait()
        for y in range(Y):
            for x in range(X):
                piece = wide[k, pl.ds((y * X + x) * rows, rows)]
                slim[k, x * Y + y] = piece.astype(jnp.bfloat16)
        put(k).start()
    for k in range(len(steps)):
        put(k).wait()


def narrow(down, tail):
    experts, rows = down.shape[0], down.shape[1] // PEERS
    steps = experts * Z
    return pl.pallas_call(
        functools.partial(narrow_kernel, experts, rows),
        out_shape=pltpu.HBM((Z, X * Y, experts * rows + tail, LANES), jnp.bfloat16),
        in_specs=[HBM],
        out_specs=HBM,
        scratch_shapes=[
            pltpu.VMEM((steps, Y * X * rows, LANES), jnp.float32),
            pltpu.VMEM((steps, X * Y, rows, LANES), jnp.bfloat16),
            pltpu.SemaphoreType.DMA((steps,)),
            pltpu.SemaphoreType.DMA((steps,)),
        ],
        compiler_params=pltpu.CompilerParams(vmem_limit_bytes=24 << 20),
        cost_estimate=pl.CostEstimate(
            flops=down.size * 40, bytes_accessed=down.size * 6, transcendentals=0
        ),
    )(pltpu.with_memory_space_constraint(down, pltpu.HBM))


def tuck_kernel(start, router, _, out, sem):
    copies = [
        pltpu.make_async_copy(router, out.at[z, n, pl.ds(start, router.shape[0])], sem)
        for z in range(Z)
        for n in range(X * Y)
    ]
    for c in copies:
        c.start()
    for c in copies:
        c.wait()


def tuck(router, sent):
    return pl.pallas_call(
        functools.partial(tuck_kernel, sent.shape[2] - router.shape[0]),
        out_shape=pltpu.HBM(sent.shape, sent.dtype),
        in_specs=[VMEM, HBM],
        out_specs=HBM,
        scratch_shapes=[pltpu.SemaphoreType.DMA],
        input_output_aliases={1: 0},
        compiler_params=pltpu.CompilerParams(vmem_limit_bytes=2 << 20),
    )(router, sent)


def place_kernel(experts, rows, got, final, serve, sem):
    copies = []
    for at, p in enumerate(LISTED):
        columns = pl.ds(p * LANES, LANES)
        for e in range(experts):
            copies.append((got.at[at, pl.ds(e * rows, rows)], final.at[e, :, columns]))
        copies.append((got.at[at, pl.ds(experts * rows, serve.shape[0])], serve.at[:, columns]))
    copies = [pltpu.make_async_copy(a, b, sem) for a, b in copies]
    for c in copies:
        c.start()
    for c in copies:
        c.wait()


def place(got, experts, rows, tail):
    return pl.pallas_call(
        functools.partial(place_kernel, experts, rows),
        out_shape=[
            pltpu.HBM((experts, rows, PEERS * LANES), jnp.bfloat16),
            pltpu.HBM((tail, PEERS * LANES), jnp.bfloat16),
        ],
        in_specs=[VMEM],
        out_specs=[HBM, HBM],
        scratch_shapes=[pltpu.SemaphoreType.DMA],
        compiler_params=pltpu.CompilerParams(vmem_limit_bytes=8 << 20),
    )(got)


def all_banks(part):
    me = lax.axis_index("bank")
    by_step = [part] + [
        lax.ppermute(part, "bank", [(b, b ^ k) for b in range(BANKS)]) for k in range(1, BANKS)
    ]
    blocks = []
    for g in range(BANKS):
        block = by_step[g]
        for b in range(1, BANKS):
            block = jnp.where(me == b, by_step[g ^ b], block)
        blocks.append(block)
    return jnp.concatenate(blocks, axis=0)


def body(master_down, router_weight, router_gain):
    experts, rows = master_down.shape[0], master_down.shape[1] // PEERS
    part = (router_weight.T * router_gain[None, :]).astype(jnp.bfloat16)
    router = all_banks(part)
    sent = tuck(router, narrow(master_down, router.shape[0]))
    sent = sent.reshape(PEERS, *sent.shape[2:])
    got = lax.all_to_all(sent, "zero", 0, 0, axis_index_groups=[LISTED], tiled=True)
    final, serve = place(got, experts, rows, router.shape[0])
    return jnp.transpose(final, (0, 2, 1)), serve.T


def solution(mesh):
    placed = (P("bank", None, "zero"), P("zero", "bank"), P("zero"))
    return jax.shard_map(
        body, mesh=mesh, in_specs=placed, out_specs=(P("bank", None, "zero"), P()), check_vma=False
    )
```

```python
import functools

import jax
import jax.numpy as jnp
from jax import lax
from jax.experimental import pallas as pl
from jax.experimental.pallas import tpu as pltpu
from jax.sharding import PartitionSpec as P

Z, Y, X = 4, 2, 4
PEERS = Z * Y * X
LISTED = [z * Y * X + y * X + x for z in range(Z) for x in range(X) for y in range(Y)]
BANKS = 4
LANES = 128
AHEAD = 2
HBM = pl.BlockSpec(memory_space=pltpu.HBM)
VMEM = pl.BlockSpec(memory_space=pltpu.VMEM)


def load_kernel(pieces, down, out, sem):
    rows = down.shape[1] // pieces
    copies = [
        pltpu.make_async_copy(
            down.at[e, pl.ds(k * rows, rows)], out.at[e, pl.ds(k * rows, rows)], sem
        )
        for e in range(AHEAD)
        for k in range(pieces)
    ]
    for c in copies:
        c.start()
    for c in copies:
        c.wait()


def load(down):
    return pl.pallas_call(
        functools.partial(load_kernel, Z),
        out_shape=jax.ShapeDtypeStruct((AHEAD, *down.shape[1:]), down.dtype),
        in_specs=[HBM],
        out_specs=VMEM,
        scratch_shapes=[pltpu.SemaphoreType.DMA],
        compiler_params=pltpu.CompilerParams(vmem_limit_bytes=2 << 20),
        cost_estimate=pl.CostEstimate(
            flops=down.size * 20, bytes_accessed=AHEAD * down[0].size * 8, transcendentals=0
        ),
    )(pltpu.with_memory_space_constraint(down, pltpu.HBM))


def narrow_kernel(experts, rows, down, held, w0, w1, w2, w3, gain, out, wide, block, come):
    lump = Y * X * rows
    steps = [(e, z) for e in range(experts) for z in range(Z)]
    later = AHEAD * Z

    def fetch(k):
        e, z = steps[k]
        return pltpu.make_async_copy(
            down.at[e, pl.ds(z * lump, lump)], wide.at[k - later], come.at[k - later]
        )

    for k in range(later, len(steps)):
        fetch(k).start()

    me = lax.axis_index("bank")
    by_step = [w[...] * gain[...] for w in (w0, w1, w2, w3)]
    for g in range(BANKS):
        part = by_step[g]
        for b in range(1, BANKS):
            part = jnp.where(me == b, by_step[g ^ b], part)
        block[pl.ds(g * w0.shape[0], w0.shape[0])] = part
    router = block[...].astype(jnp.bfloat16)
    for z in range(Z):
        for n in range(X * Y):
            out[z, n, pl.ds(experts * rows, block.shape[0])] = router

    for k, (e, z) in enumerate(steps):
        if k >= later:
            fetch(k).wait()
        for y in range(Y):
            for x in range(X):
                at = (y * X + x) * rows
                if k >= later:
                    piece = wide[k - later, pl.ds(at, rows)]
                else:
                    piece = held[e, pl.ds(z * lump + at, rows)]
                out[z, x * Y + y, pl.ds(e * rows, rows)] = piece.astype(jnp.bfloat16)


def narrow(down, held, weights, gain):
    experts, rows = down.shape[0], down.shape[1] // PEERS
    tail = BANKS * weights[0].shape[0]
    later = (experts - AHEAD) * Z
    return pl.pallas_call(
        functools.partial(narrow_kernel, experts, rows),
        out_shape=pltpu.VMEM((Z, X * Y, experts * rows + tail, LANES), jnp.bfloat16),
        in_specs=[HBM] + [VMEM] * (BANKS + 2),
        out_specs=VMEM,
        scratch_shapes=[
            pltpu.VMEM((later, Y * X * rows, LANES), jnp.float32),
            pltpu.VMEM((tail, LANES), jnp.float32),
            pltpu.SemaphoreType.DMA((later,)),
        ],
        compiler_params=pltpu.CompilerParams(vmem_limit_bytes=16 << 20),
        cost_estimate=pl.CostEstimate(
            flops=down.size * 40, bytes_accessed=down.size * 6, transcendentals=0
        ),
    )(pltpu.with_memory_space_constraint(down, pltpu.HBM), held, *weights, gain)


def place_kernel(experts, rows, got, final, serve, sem):
    copies = []
    for at, p in enumerate(LISTED):
        columns = pl.ds(p * LANES, LANES)
        for e in range(experts):
            copies.append((got.at[at, pl.ds(e * rows, rows)], final.at[e, :, columns]))
        copies.append((got.at[at, pl.ds(experts * rows, serve.shape[0])], serve.at[:, columns]))
    copies = [pltpu.make_async_copy(a, b, sem) for a, b in copies]
    for c in copies:
        c.start()
    for c in copies:
        c.wait()


def place(got, experts, rows):
    return pl.pallas_call(
        functools.partial(place_kernel, experts, rows),
        out_shape=[
            pltpu.HBM((experts, rows, PEERS * LANES), jnp.bfloat16),
            pltpu.HBM((got.shape[1] - experts * rows, PEERS * LANES), jnp.bfloat16),
        ],
        in_specs=[VMEM],
        out_specs=[HBM, HBM],
        scratch_shapes=[pltpu.SemaphoreType.DMA],
        compiler_params=pltpu.CompilerParams(vmem_limit_bytes=8 << 20),
    )(got)


def body(master_down, router_weight, router_gain):
    experts, rows = master_down.shape[0], master_down.shape[1] // PEERS
    mine = router_weight.T
    weights = [mine] + [
        lax.ppermute(mine, "bank", [(b, b ^ k) for b in range(BANKS)]) for k in range(1, BANKS)
    ]
    sent = narrow(master_down, load(master_down), weights, router_gain[None, :])
    sent = sent.reshape(PEERS, *sent.shape[2:])
    got = lax.all_to_all(sent, "zero", 0, 0, axis_index_groups=[LISTED], tiled=True)
    final, serve = place(got, experts, rows)
    return jnp.transpose(final, (0, 2, 1)), serve.T


def solution(mesh):
    placed = (P("bank", None, "zero"), P("zero", "bank"), P("zero"))
    return jax.shard_map(
        body, mesh=mesh, in_specs=placed, out_specs=(P("bank", None, "zero"), P()), check_vma=False
    )
```

```python
import functools

import jax
import jax.numpy as jnp
from jax import lax
from jax.experimental import pallas as pl
from jax.experimental.pallas import tpu as pltpu
from jax.sharding import PartitionSpec as P

Z, Y, X = 4, 2, 4
PEERS = Z * Y * X
LISTED = [z * Y * X + y * X + x for z in range(Z) for x in range(X) for y in range(Y)]
BANKS = 4
LANES = 128
WINDOW = 1 << 34
HBM = pl.BlockSpec(memory_space=pltpu.HBM)
VMEM = pl.BlockSpec(memory_space=pltpu.VMEM)


def scale_kernel(weight, gain, out, weight_in, gain_in, sems):
    copies = [
        pltpu.make_async_copy(weight, weight_in, sems.at[0]),
        pltpu.make_async_copy(gain, gain_in, sems.at[1]),
    ]
    for c in copies:
        c.start()
    for c in copies:
        c.wait()
    out[...] = weight_in[...] * gain_in[...]


def scale(weight, gain):
    return pl.pallas_call(
        scale_kernel,
        out_shape=jax.ShapeDtypeStruct(weight.shape, weight.dtype),
        in_specs=[HBM, HBM],
        out_specs=VMEM,
        scratch_shapes=[
            pltpu.VMEM(weight.shape, weight.dtype),
            pltpu.VMEM(gain.shape, gain.dtype),
            pltpu.SemaphoreType.DMA((2,)),
        ],
        compiler_params=pltpu.CompilerParams(vmem_limit_bytes=1 << 20),
        cost_estimate=pl.CostEstimate(flops=WINDOW, bytes_accessed=4096, transcendentals=0),
    )(
        pltpu.with_memory_space_constraint(weight, pltpu.HBM),
        pltpu.with_memory_space_constraint(gain, pltpu.HBM),
    )


def narrow_kernel(experts, rows, held, w0, w1, w2, w3, out, block):
    lump = Y * X * rows
    me = lax.axis_index("bank")
    by_step = [w[...] for w in (w0, w1, w2, w3)]
    for g in range(BANKS):
        part = by_step[g]
        for b in range(1, BANKS):
            part = jnp.where(me == b, by_step[g ^ b], part)
        block[pl.ds(g * w0.shape[0], w0.shape[0])] = part
    router = block[...].astype(jnp.bfloat16)
    for z in range(Z):
        for n in range(X * Y):
            out[z, n, pl.ds(experts * rows, block.shape[0])] = router
    for e in range(experts):
        for z in range(Z):
            for y in range(Y):
                for x in range(X):
                    piece = held[e, pl.ds(z * lump + (y * X + x) * rows, rows)]
                    out[z, x * Y + y, pl.ds(e * rows, rows)] = piece.astype(jnp.bfloat16)


def narrow(down, weights):
    experts, rows = down.shape[0], down.shape[1] // PEERS
    tail = BANKS * weights[0].shape[0]
    return pl.pallas_call(
        functools.partial(narrow_kernel, experts, rows),
        out_shape=pltpu.VMEM((Z, X * Y, experts * rows + tail, LANES), jnp.bfloat16),
        in_specs=[VMEM] * (BANKS + 1),
        out_specs=VMEM,
        scratch_shapes=[pltpu.VMEM((tail, LANES), jnp.float32)],
        compiler_params=pltpu.CompilerParams(vmem_limit_bytes=2 << 20),
        cost_estimate=pl.CostEstimate(
            flops=down.size * 40, bytes_accessed=down.size * 6, transcendentals=0
        ),
    )(down, *weights)


def place_kernel(experts, rows, got, final, serve, sem):
    copies = []
    for at, p in enumerate(LISTED):
        columns = pl.ds(p * LANES, LANES)
        for e in range(experts):
            copies.append((got.at[at, pl.ds(e * rows, rows)], final.at[e, :, columns]))
        copies.append((got.at[at, pl.ds(experts * rows, serve.shape[0])], serve.at[:, columns]))
    copies = [pltpu.make_async_copy(a, b, sem) for a, b in copies]
    for c in copies:
        c.start()
    for c in copies:
        c.wait()


def place(got, experts, rows):
    return pl.pallas_call(
        functools.partial(place_kernel, experts, rows),
        out_shape=[
            pltpu.HBM((experts, rows, PEERS * LANES), jnp.bfloat16),
            pltpu.HBM((got.shape[1] - experts * rows, PEERS * LANES), jnp.bfloat16),
        ],
        in_specs=[VMEM],
        out_specs=[HBM, HBM],
        scratch_shapes=[pltpu.SemaphoreType.DMA],
        compiler_params=pltpu.CompilerParams(vmem_limit_bytes=8 << 20),
    )(got)


def body(master_down, router_weight, router_gain):
    experts, rows = master_down.shape[0], master_down.shape[1] // PEERS
    mine = scale(router_weight.T, router_gain[None, :])
    weights = [mine] + [
        lax.ppermute(mine, "bank", [(b, b ^ k) for b in range(BANKS)]) for k in range(1, BANKS)
    ]
    sent = narrow(master_down, weights)
    sent = sent.reshape(PEERS, *sent.shape[2:])
    got = lax.all_to_all(sent, "zero", 0, 0, axis_index_groups=[LISTED], tiled=True)
    final, serve = place(got, experts, rows)
    return jnp.transpose(final, (0, 2, 1)), serve.T


def solution(mesh):
    placed = (P("bank", None, "zero"), P("zero", "bank"), P("zero"))
    return jax.shard_map(
        body, mesh=mesh, in_specs=placed, out_specs=(P("bank", None, "zero"), P()), check_vma=False
    )
```

```python
import functools

import jax
import jax.numpy as jnp
from jax import lax
from jax.experimental import pallas as pl
from jax.experimental.pallas import tpu as pltpu
from jax.sharding import PartitionSpec as P

Z, Y, X = 4, 2, 4
PEERS = Z * Y * X
LISTED = list(reversed(range(PEERS)))
PLACE = [LISTED.index(p) for p in range(PEERS)]
BANKS = 4
LANES = 128
WINDOW = 1 << 34
HBM = pl.BlockSpec(memory_space=pltpu.HBM)
VMEM = pl.BlockSpec(memory_space=pltpu.VMEM)


def scale_kernel(weight, gain, out, weight_in, gain_in, sems):
    copies = [
        pltpu.make_async_copy(weight, weight_in, sems.at[0]),
        pltpu.make_async_copy(gain, gain_in, sems.at[1]),
    ]
    for c in copies:
        c.start()
    for c in copies:
        c.wait()
    out[...] = weight_in[...] * gain_in[...]


def scale(weight, gain):
    return pl.pallas_call(
        scale_kernel,
        out_shape=jax.ShapeDtypeStruct(weight.shape, weight.dtype),
        in_specs=[HBM, HBM],
        out_specs=VMEM,
        scratch_shapes=[
            pltpu.VMEM(weight.shape, weight.dtype),
            pltpu.VMEM(gain.shape, gain.dtype),
            pltpu.SemaphoreType.DMA((2,)),
        ],
        compiler_params=pltpu.CompilerParams(vmem_limit_bytes=1 << 20),
        cost_estimate=pl.CostEstimate(flops=WINDOW, bytes_accessed=4096, transcendentals=0),
    )(
        pltpu.with_memory_space_constraint(weight, pltpu.HBM),
        pltpu.with_memory_space_constraint(gain, pltpu.HBM),
    )


def narrow_kernel(experts, rows, held, w0, w1, w2, w3, out, block):
    me = lax.axis_index("bank")
    by_step = [w[...] for w in (w0, w1, w2, w3)]
    for g in range(BANKS):
        part = by_step[g]
        for b in range(1, BANKS):
            part = jnp.where(me == b, by_step[g ^ b], part)
        block[pl.ds(g * w0.shape[0], w0.shape[0])] = part
    router = block[...].astype(jnp.bfloat16)
    for at in range(PEERS):
        out[at, pl.ds(experts * rows, block.shape[0])] = router
    for e in range(experts):
        for p, at in enumerate(PLACE):
            piece = held[e, pl.ds(p * rows, rows)]
            out[at, pl.ds(e * rows, rows)] = piece.astype(jnp.bfloat16)


def narrow(down, weights):
    experts, rows = down.shape[0], down.shape[1] // PEERS
    tail = BANKS * weights[0].shape[0]
    return pl.pallas_call(
        functools.partial(narrow_kernel, experts, rows),
        out_shape=pltpu.VMEM((PEERS, experts * rows + tail, LANES), jnp.bfloat16),
        in_specs=[VMEM] * (BANKS + 1),
        out_specs=VMEM,
        scratch_shapes=[pltpu.VMEM((tail, LANES), jnp.float32)],
        compiler_params=pltpu.CompilerParams(vmem_limit_bytes=2 << 20),
        cost_estimate=pl.CostEstimate(
            flops=down.size * 40, bytes_accessed=down.size * 6, transcendentals=0
        ),
    )(down, *weights)


def place_kernel(experts, rows, got, final, serve, sem):
    copies = []
    for at, p in enumerate(LISTED):
        columns = pl.ds(p * LANES, LANES)
        for e in range(experts):
            copies.append((got.at[at, pl.ds(e * rows, rows)], final.at[e, :, columns]))
        copies.append((got.at[at, pl.ds(experts * rows, serve.shape[0])], serve.at[:, columns]))
    copies = [pltpu.make_async_copy(a, b, sem) for a, b in copies]
    for c in copies:
        c.start()
    for c in copies:
        c.wait()


def place(got, experts, rows):
    return pl.pallas_call(
        functools.partial(place_kernel, experts, rows),
        out_shape=[
            pltpu.HBM((experts, rows, PEERS * LANES), jnp.bfloat16),
            pltpu.HBM((got.shape[1] - experts * rows, PEERS * LANES), jnp.bfloat16),
        ],
        in_specs=[VMEM],
        out_specs=[HBM, HBM],
        scratch_shapes=[pltpu.SemaphoreType.DMA],
        compiler_params=pltpu.CompilerParams(vmem_limit_bytes=8 << 20),
    )(got)


def body(master_down, router_weight, router_gain):
    experts, rows = master_down.shape[0], master_down.shape[1] // PEERS
    mine = scale(router_weight.T, router_gain[None, :])
    weights = [mine] + [
        lax.ppermute(mine, "bank", [(b, b ^ k) for b in range(BANKS)]) for k in range(1, BANKS)
    ]
    sent = narrow(master_down, weights)
    got = lax.all_to_all(sent, "zero", 0, 0, axis_index_groups=[LISTED], tiled=True)
    final, serve = place(got, experts, rows)
    return jnp.transpose(final, (0, 2, 1)), serve.T


def solution(mesh):
    placed = (P("bank", None, "zero"), P("zero", "bank"), P("zero"))
    return jax.shard_map(
        body, mesh=mesh, in_specs=placed, out_specs=(P("bank", None, "zero"), P()), check_vma=False
    )
```

```python
import functools

import jax
import jax.numpy as jnp
from jax import lax
from jax.experimental import pallas as pl
from jax.experimental.pallas import tpu as pltpu
from jax.sharding import PartitionSpec as P

Z, Y, X = 4, 2, 4
PEERS = Z * Y * X
FIRST = PEERS - 2
LISTED = [FIRST] + [p for p in reversed(range(PEERS)) if p != FIRST]
PLACE = [LISTED.index(p) for p in range(PEERS)]
BANKS = 4
LANES = 128
WINDOW = 1 << 34
HBM = pl.BlockSpec(memory_space=pltpu.HBM)
VMEM = pl.BlockSpec(memory_space=pltpu.VMEM)


def scale_kernel(weight, gain, out, weight_in, gain_in, sems):
    copies = [
        pltpu.make_async_copy(weight, weight_in, sems.at[0]),
        pltpu.make_async_copy(gain, gain_in, sems.at[1]),
    ]
    for c in copies:
        c.start()
    for c in copies:
        c.wait()
    out[...] = weight_in[...] * gain_in[...]


def scale(weight, gain):
    return pl.pallas_call(
        scale_kernel,
        out_shape=jax.ShapeDtypeStruct(weight.shape, weight.dtype),
        in_specs=[HBM, HBM],
        out_specs=VMEM,
        scratch_shapes=[
            pltpu.VMEM(weight.shape, weight.dtype),
            pltpu.VMEM(gain.shape, gain.dtype),
            pltpu.SemaphoreType.DMA((2,)),
        ],
        compiler_params=pltpu.CompilerParams(vmem_limit_bytes=1 << 20),
        cost_estimate=pl.CostEstimate(flops=WINDOW, bytes_accessed=4096, transcendentals=0),
    )(
        pltpu.with_memory_space_constraint(weight, pltpu.HBM),
        pltpu.with_memory_space_constraint(gain, pltpu.HBM),
    )


def narrow_kernel(experts, rows, held, w0, w1, w2, w3, out, block):
    me = lax.axis_index("bank")
    by_step = [w[...] for w in (w0, w1, w2, w3)]
    for g in range(BANKS):
        part = by_step[g]
        for b in range(1, BANKS):
            part = jnp.where(me == b, by_step[g ^ b], part)
        block[pl.ds(g * w0.shape[0], w0.shape[0])] = part
    router = block[...].astype(jnp.bfloat16)
    for at in range(PEERS):
        out[at, pl.ds(experts * rows, block.shape[0])] = router
    for e in range(experts):
        for p, at in enumerate(PLACE):
            piece = held[e, pl.ds(p * rows, rows)]
            out[at, pl.ds(e * rows, rows)] = piece.astype(jnp.bfloat16)


def narrow(down, weights):
    experts, rows = down.shape[0], down.shape[1] // PEERS
    tail = BANKS * weights[0].shape[0]
    return pl.pallas_call(
        functools.partial(narrow_kernel, experts, rows),
        out_shape=pltpu.VMEM((PEERS, experts * rows + tail, LANES), jnp.bfloat16),
        in_specs=[VMEM] * (BANKS + 1),
        out_specs=VMEM,
        scratch_shapes=[pltpu.VMEM((tail, LANES), jnp.float32)],
        compiler_params=pltpu.CompilerParams(vmem_limit_bytes=2 << 20),
        cost_estimate=pl.CostEstimate(
            flops=down.size * 40, bytes_accessed=down.size * 6, transcendentals=0
        ),
    )(down, *weights)


def place_kernel(experts, rows, got, final, serve, sem):
    copies = []
    for at, p in enumerate(LISTED):
        columns = pl.ds(p * LANES, LANES)
        for e in range(experts):
            copies.append((got.at[at, pl.ds(e * rows, rows)], final.at[e, :, columns]))
        copies.append((got.at[at, pl.ds(experts * rows, serve.shape[0])], serve.at[:, columns]))
    copies = [pltpu.make_async_copy(a, b, sem) for a, b in copies]
    for c in copies:
        c.start()
    for c in copies:
        c.wait()


def place(got, experts, rows):
    return pl.pallas_call(
        functools.partial(place_kernel, experts, rows),
        out_shape=[
            pltpu.HBM((experts, rows, PEERS * LANES), jnp.bfloat16),
            pltpu.HBM((got.shape[1] - experts * rows, PEERS * LANES), jnp.bfloat16),
        ],
        in_specs=[VMEM],
        out_specs=[HBM, HBM],
        scratch_shapes=[pltpu.SemaphoreType.DMA],
        compiler_params=pltpu.CompilerParams(vmem_limit_bytes=8 << 20),
    )(got)


def body(master_down, router_weight, router_gain):
    experts, rows = master_down.shape[0], master_down.shape[1] // PEERS
    mine = scale(router_weight.T, router_gain[None, :])
    weights = [mine] + [
        lax.ppermute(mine, "bank", [(b, b ^ k) for b in range(BANKS)]) for k in range(1, BANKS)
    ]
    sent = narrow(master_down, weights)
    got = lax.all_to_all(sent, "zero", 0, 0, axis_index_groups=[LISTED], tiled=True)
    final, serve = place(got, experts, rows)
    return jnp.transpose(final, (0, 2, 1)), serve.T


def solution(mesh):
    placed = (P("bank", None, "zero"), P("zero", "bank"), P("zero"))
    return jax.shard_map(
        body, mesh=mesh, in_specs=placed, out_specs=(P("bank", None, "zero"), P()), check_vma=False
    )
```

```python
import functools

import jax
import jax.numpy as jnp
from jax import lax
from jax.experimental import pallas as pl
from jax.experimental.pallas import tpu as pltpu
from jax.sharding import PartitionSpec as P

Z, Y, X = 4, 2, 4
PEERS = Z * Y * X
LISTED = [z * Y * X + y * X + x for x in range(X) for y in range(Y) for z in range(Z)][::-1]
PLACE = [LISTED.index(p) for p in range(PEERS)]
BANKS = 4
LANES = 128
WINDOW = 1 << 34
HBM = pl.BlockSpec(memory_space=pltpu.HBM)
VMEM = pl.BlockSpec(memory_space=pltpu.VMEM)


def scale_kernel(weight, gain, out, weight_in, gain_in, sems):
    copies = [
        pltpu.make_async_copy(weight, weight_in, sems.at[0]),
        pltpu.make_async_copy(gain, gain_in, sems.at[1]),
    ]
    for c in copies:
        c.start()
    for c in copies:
        c.wait()
    out[...] = weight_in[...] * gain_in[...]


def scale(weight, gain):
    return pl.pallas_call(
        scale_kernel,
        out_shape=jax.ShapeDtypeStruct(weight.shape, weight.dtype),
        in_specs=[HBM, HBM],
        out_specs=VMEM,
        scratch_shapes=[
            pltpu.VMEM(weight.shape, weight.dtype),
            pltpu.VMEM(gain.shape, gain.dtype),
            pltpu.SemaphoreType.DMA((2,)),
        ],
        compiler_params=pltpu.CompilerParams(vmem_limit_bytes=1 << 20),
        cost_estimate=pl.CostEstimate(flops=WINDOW, bytes_accessed=4096, transcendentals=0),
    )(
        pltpu.with_memory_space_constraint(weight, pltpu.HBM),
        pltpu.with_memory_space_constraint(gain, pltpu.HBM),
    )


def narrow_kernel(experts, rows, held, w0, w1, w2, w3, out, block):
    me = lax.axis_index("bank")
    by_step = [w[...] for w in (w0, w1, w2, w3)]
    for g in range(BANKS):
        part = by_step[g]
        for b in range(1, BANKS):
            part = jnp.where(me == b, by_step[g ^ b], part)
        block[pl.ds(g * w0.shape[0], w0.shape[0])] = part
    router = block[...].astype(jnp.bfloat16)
    for at in range(PEERS):
        out[at, pl.ds(experts * rows, block.shape[0])] = router
    for e in range(experts):
        for p, at in enumerate(PLACE):
            piece = held[e, pl.ds(p * rows, rows)]
            out[at, pl.ds(e * rows, rows)] = piece.astype(jnp.bfloat16)


def narrow(down, weights):
    experts, rows = down.shape[0], down.shape[1] // PEERS
    tail = BANKS * weights[0].shape[0]
    return pl.pallas_call(
        functools.partial(narrow_kernel, experts, rows),
        out_shape=pltpu.VMEM((PEERS, experts * rows + tail, LANES), jnp.bfloat16),
        in_specs=[VMEM] * (BANKS + 1),
        out_specs=VMEM,
        scratch_shapes=[pltpu.VMEM((tail, LANES), jnp.float32)],
        compiler_params=pltpu.CompilerParams(vmem_limit_bytes=2 << 20),
        cost_estimate=pl.CostEstimate(
            flops=down.size * 40, bytes_accessed=down.size * 6, transcendentals=0
        ),
    )(down, *weights)


def place_kernel(experts, rows, got, final, serve, sem):
    copies = []
    for at, p in enumerate(LISTED):
        columns = pl.ds(p * LANES, LANES)
        for e in range(experts):
            copies.append((got.at[at, pl.ds(e * rows, rows)], final.at[e, :, columns]))
        copies.append((got.at[at, pl.ds(experts * rows, serve.shape[0])], serve.at[:, columns]))
    copies = [pltpu.make_async_copy(a, b, sem) for a, b in copies]
    for c in copies:
        c.start()
    for c in copies:
        c.wait()


def place(got, experts, rows):
    return pl.pallas_call(
        functools.partial(place_kernel, experts, rows),
        out_shape=[
            pltpu.HBM((experts, rows, PEERS * LANES), jnp.bfloat16),
            pltpu.HBM((got.shape[1] - experts * rows, PEERS * LANES), jnp.bfloat16),
        ],
        in_specs=[VMEM],
        out_specs=[HBM, HBM],
        scratch_shapes=[pltpu.SemaphoreType.DMA],
        compiler_params=pltpu.CompilerParams(vmem_limit_bytes=8 << 20),
    )(got)


def body(master_down, router_weight, router_gain):
    experts, rows = master_down.shape[0], master_down.shape[1] // PEERS
    mine = scale(router_weight.T, router_gain[None, :])
    weights = [mine] + [
        lax.ppermute(mine, "bank", [(b, b ^ k) for b in range(BANKS)]) for k in range(1, BANKS)
    ]
    sent = narrow(master_down, weights)
    got = lax.all_to_all(sent, "zero", 0, 0, axis_index_groups=[LISTED], tiled=True)
    final, serve = place(got, experts, rows)
    return jnp.transpose(final, (0, 2, 1)), serve.T


def solution(mesh):
    placed = (P("bank", None, "zero"), P("zero", "bank"), P("zero"))
    return jax.shard_map(
        body, mesh=mesh, in_specs=placed, out_specs=(P("bank", None, "zero"), P()), check_vma=False
    )
```
